32 devices in a mesh: gx: 16 (over z, y, x), yz: 2 (over core).
Axes of the slice: x: 2, y: 2, z: 4, core: 2. Of those that a mesh axis runs over, the one named last changes fastest.
Arguments:
- magnet: bfloat16 [256, 3, 16, 256], P('yz', None, 'gx'), may hold values from -5 to 5
- newell: bfloat16 [256, 6, 16, 256], P('yz'), may hold values from -0.875 to 0.875
Outputs:
- field: bfloat16 [256, 3, 16, 256], P('yz', None, 'gx')
The draws below stay inside these ranges and needn't reach their ends.
All inputs are finite; a program needn't handle non-finite values.
Results may differ from the reference program's by a relative error of at most 0.0055.
Values may be sent and summed in bfloat16 or wider, within the bound.
A program may use at most 256 MiB of HBM per device.

```python
import math
import jax
import jax.numpy as jnp
from jax import lax

NY = 256
NZ = 256
NX = 16


def steps_of(key, extent, cuts, least, high):
    level, own = 1.0, jax.random.fold_in(key, 6)
    for position, parts in cuts:
        steps = jnp.exp(jax.random.uniform(jax.random.fold_in(own, position), (parts,), jnp.float32, least / len(cuts), high / len(cuts)))
        level = level * jnp.repeat(steps, extent[position] // parts).reshape([-1 if axis == position else 1 for axis in range(len(extent))])
    return level


def scatter_about(key, shape, scale, bound, pieces=(), held_as=jnp.bfloat16):
    level = steps_of(key, shape, pieces, -0.22, 0.18) if pieces else 1.0
    array = jax.random.normal(key, shape, jnp.float32) * scale * level
    return jnp.minimum(jnp.maximum(array, -bound), bound).astype(held_as)


def setup_inputs(seed: int = 0) -> dict:
    arg_keys = jax.random.split(jax.random.key(seed), 3)
    magnet = scatter_about(arg_keys[0], (NY, 3, NX, NZ), 1.0, 5.0, ((0, 2), (2, 16)))
    newell = scatter_about(arg_keys[1], (NY, 6, NX, NZ), (3 * NX) ** -0.5, 0.875, ((0, 2),))
    return {"magnet": magnet, "newell": newell}


EXCHANGE = 0.2


def dft_tables(row_count, col_count, length, row_first, col_first):
    row_ids = (row_first + jnp.arange(row_count, dtype=jnp.int32))[:, None]
    col_ids = (col_first + jnp.arange(col_count, dtype=jnp.int32))[None, :]
    angles = ((row_ids * col_ids) % length).astype(jnp.float32) * (2.0 * math.pi / length)
    return jnp.cos(angles).astype(jnp.bfloat16), jnp.sin(angles).astype(jnp.bfloat16)


def forward_y(z_rows, cos_y, sin_y):
    half_cols = z_rows.shape[-1] // 2
    cos_part = jnp.einsum("ky,ycxq->kcxq", cos_y.astype(jnp.float32), z_rows.astype(jnp.float32))
    sin_part = jnp.einsum("ky,ycxq->kcxq", sin_y.astype(jnp.float32), z_rows.astype(jnp.float32))
    return jnp.concatenate([cos_part[..., :half_cols] + sin_part[..., half_cols:], cos_part[..., half_cols:] - sin_part[..., :half_cols]], axis=-1)


def inverse_y(modes_in, cos_y, sin_y):
    half_cols = modes_in.shape[-1] // 2
    cos_part = jnp.einsum("yk,kcxq->ycxq", cos_y.astype(jnp.float32), modes_in.astype(jnp.float32))
    sin_part = jnp.einsum("yk,kcxq->ycxq", sin_y.astype(jnp.float32), modes_in.astype(jnp.float32))
    return jnp.concatenate([cos_part[..., :half_cols] - sin_part[..., half_cols:], cos_part[..., half_cols:] + sin_part[..., :half_cols]], axis=-1)


def convolve(kernel_rows, source, tgt_first, tgt_rows, src_first):
    src_rows = source.shape[2]
    half_cols = source.shape[3] // 2
    modes = source.shape[0]
    offset = (tgt_first + jnp.arange(tgt_rows, dtype=jnp.int32))[:, None] - (src_first + jnp.arange(src_rows, dtype=jnp.int32))[None, :]
    distance = jnp.abs(offset).astype(jnp.int32)
    sign_flip = jnp.where(offset >= 0, 1.0, -1.0).astype(jnp.float32)[None, :, :, None]
    picked = jnp.take(kernel_rows, distance.reshape(-1), axis=2).reshape(modes, 6, tgt_rows, src_rows, half_cols)

    def mix_term(kern_comp, source_comp, imag_part, signed):
        weight = picked[:, kern_comp].astype(jnp.float32)
        if signed:
            weight = weight * sign_flip
        if imag_part:
            values = source[:, source_comp, :, half_cols:]
        else:
            values = source[:, source_comp, :, :half_cols]
        return jnp.sum(weight * values.astype(jnp.float32)[:, None], axis=2)

    x_real = -(mix_term(0, 0, False, False) - mix_term(4, 1, True, True) - mix_term(5, 2, True, True))
    x_imag = -(mix_term(0, 0, True, False) + mix_term(4, 1, False, True) + mix_term(5, 2, False, True))
    y_real = -(-mix_term(4, 0, True, True) + mix_term(1, 1, False, False) + mix_term(3, 2, False, False))
    y_imag = -(mix_term(4, 0, False, True) + mix_term(1, 1, True, False) + mix_term(3, 2, True, False))
    z_real = -(-mix_term(5, 0, True, True) + mix_term(3, 1, False, False) + mix_term(2, 2, False, False))
    z_imag = -(mix_term(5, 0, False, True) + mix_term(3, 1, True, False) + mix_term(2, 2, True, False))
    return jnp.stack([jnp.concatenate([x_real, x_imag], axis=-1), jnp.concatenate([y_real, y_imag], axis=-1), jnp.concatenate([z_real, z_imag], axis=-1)], axis=1)


def block_conv(pairing):
    return convolve(pairing[0], pairing[1], 0, NX, 0)


def reference(magnet, newell):
    cos_z, sin_z = dft_tables(NZ, NZ, NZ, 0, 0)
    cos_y, sin_y = dft_tables(NY, NY, NY, 0, 0)
    forward_z = jnp.concatenate([cos_z, -sin_z], axis=1)
    z_rows = jnp.dot(magnet, forward_z, preferred_element_type=jnp.float32).astype(jnp.bfloat16)
    spectrum = forward_y(z_rows, cos_y, sin_y).astype(jnp.bfloat16)
    blocks = NY // 8
    spec_blocks = spectrum.reshape(blocks, 8, 3, NX, 2 * NZ)
    table_blocks = newell.reshape(blocks, 8, 6, NX, NZ)
    field_blocks = lax.map(block_conv, (table_blocks, spec_blocks))
    field_spec = field_blocks.reshape(NY, 3, NX, 2 * NZ).astype(jnp.bfloat16)
    g_rows = inverse_y(field_spec, cos_y, sin_y).astype(jnp.bfloat16)
    inverse_z = jnp.concatenate([cos_z, -sin_z], axis=0)
    demag_field = jnp.dot(g_rows, inverse_z, preferred_element_type=jnp.float32) / (NY * NZ)
    centre = magnet.astype(jnp.float32)
    step_x = centre[:, :, 1:] - centre[:, :, :-1]
    laplace = jnp.pad(step_x, ((0, 0), (0, 0), (0, 1), (0, 0))) - jnp.pad(step_x, ((0, 0), (0, 0), (1, 0), (0, 0)))
    laplace = laplace + jnp.roll(centre, 1, 0) + jnp.roll(centre, -1, 0) - 2.0 * centre
    laplace = laplace + jnp.roll(centre, 1, 3) + jnp.roll(centre, -1, 3) - 2.0 * centre
    return (demag_field + EXCHANGE * laplace).astype(jnp.bfloat16)
```

```python
import functools
import math

import jax
import jax.numpy as jnp
import ml_dtypes
import numpy as np
from jax import lax
from jax.experimental import pallas as pl
from jax.experimental.pallas import tpu as pltpu
from jax.sharding import PartitionSpec as P

EXCHANGE = 0.2
F32 = jnp.float32
BF16 = jnp.bfloat16
MESH = pl.DeviceIdType.MESH


def ky_owned(groups, parts, pairs, length):
    order = []
    for part in range(parts):
        for g in range(groups):
            first = [(g * parts + part) * pairs + p for p in range(pairs)]
            mirror = [(length - t) if t else length // 2 for t in first]
            order.append(first + mirror)
    return np.array(order).reshape(parts, -1)


def tables(groups, parts, y_total, z_total):
    pairs = y_total // (groups * parts * 2)
    rows = y_total // parts
    order = ky_owned(groups, parts, pairs, y_total)

    def trig(k, n, length):
        angle = (k[:, None] * n[None, :] % length) * (2.0 * math.pi / length)
        return np.cos(angle), np.sin(angle)

    forward, inverse = [], []
    for part in range(parts):
        own_first = (np.arange(y_total) + part * rows) % y_total
        forward.append(np.stack(trig(order[part], own_first, y_total)))
        inverse.append(np.stack(trig(own_first[:rows], order.reshape(-1), y_total)))
    half = z_total // 2
    cos, sin = trig(np.arange(z_total), np.arange(half), z_total)
    alternate = np.cos(math.pi * np.arange(z_total))
    z_fwd = np.concatenate([cos, -sin], axis=1)
    z_fwd[:, half] = alternate
    z_inv = -np.concatenate([cos, -sin], axis=1).T
    z_inv[0] = -0.5
    z_inv[half] = -0.5 * alternate
    reverse = np.zeros((z_total, half))
    for k in range(half):
        reverse[-k % z_total, k] = 1.0
    cast = lambda a: np.asarray(a, np.float32).astype(ml_dtypes.bfloat16)
    return (
        cast(np.stack(forward)),
        cast(np.stack(inverse)),
        cast(z_fwd),
        cast(z_inv),
        cast(reverse),
    )


def kernel(
    groups, pairs, magnet, newell, y_fwd, y_inv, z_fwd, z_inv, rev, out,
    mag, nwl, yf, yi, zf, zi, rv, halo, spec, send, recv, kern, source, back, fields, stack,
    lap, result, load_sem, nwl_sem, pair_sem, halo_sem, fwd_send, fwd_recv, bwd_send, bwd_recv,
    rel_send, rel_recv, out_sem,
):
    g = lax.axis_index("gx")
    c = lax.axis_index("yz")
    other = 1 - c
    own = 2 * pairs
    rows = magnet.shape[1]
    cells = groups
    half = magnet.shape[2] // 2

    barrier = pltpu.get_barrier_semaphore()
    for r in range(1, groups):
        pl.semaphore_signal(
            barrier, inc=1, device_id=(lax.rem(g + r, groups), c), device_id_type=MESH
        )
    pl.semaphore_signal(barrier, inc=1, device_id=(g, other), device_id_type=MESH)

    loads = []
    for comp in range(3):
        loads.append(
            pltpu.make_async_copy(
                magnet.at[comp], mag.at[comp, pl.ds(0, rows), :], load_sem.at[comp]
            )
        )
    loads.append(pltpu.make_async_copy(z_fwd, zf, load_sem.at[3]))
    loads.append(pltpu.make_async_copy(y_fwd.at[c], yf, load_sem.at[4]))
    loads.append(pltpu.make_async_copy(rev, rv, load_sem.at[5]))
    loads.append(pltpu.make_async_copy(y_inv.at[c], yi, load_sem.at[6]))
    loads.append(pltpu.make_async_copy(z_inv, zi, load_sem.at[7]))
    for copy in loads:
        copy.start()

    def newell_row(part, p):
        t = (2 * g + part) * pairs + p
        return (1 - c) * t + c * lax.rem(rows - t, rows)

    near = [
        pltpu.make_async_copy(newell.at[newell_row(c, p)], nwl.at[c, p], nwl_sem.at[p])
        for p in range(pairs)
    ]
    for copy in near:
        copy.start()

    pl.semaphore_wait(barrier, groups)

    for comp in range(3):
        loads[comp].wait()
    swap = []
    for comp in range(3):
        swap.append(
            pltpu.make_async_remote_copy(
                src_ref=mag.at[comp, pl.ds(0, rows), :],
                dst_ref=mag.at[comp, pl.ds(rows, rows), :],
                send_sem=pair_sem.at[0, comp],
                recv_sem=pair_sem.at[1, comp],
                device_id=(g, other),
                device_id_type=MESH,
            )
        )
    for copy in swap:
        copy.start()
    far = []
    for p in range(pairs):
        far.append(
            pltpu.make_async_remote_copy(
                src_ref=newell.at[newell_row(other, p)],
                dst_ref=nwl.at[c, p],
                send_sem=pair_sem.at[0, 3 + p],
                recv_sem=pair_sem.at[1, 3 + p],
                device_id=(g, other),
                device_id_type=MESH,
            )
        )
    for copy in far:
        copy.start()

    loads[3].wait()
    loads[4].wait()
    for comp in range(3):
        swap[comp].wait_recv()
        z_rows = jnp.dot(mag[comp], zf[...], preferred_element_type=F32).astype(BF16)
        cos_part = jnp.dot(yf[0], z_rows, preferred_element_type=F32)
        sin_part = jnp.dot(yf[1], z_rows, preferred_element_type=F32)
        low = 2 * comp * half
        spec[:, pl.ds(low, half)] = cos_part[:, :half] + sin_part[:, half:]
        spec[:, pl.ds(low + half, half)] = cos_part[:, half:] - sin_part[:, :half]
    for i in range(groups):
        send[i] = spec[pl.ds(i * own, own), :].astype(BF16)

    forward = []
    for r in range(1, groups):
        to = lax.rem(g + r, groups)
        forward.append(
            pltpu.make_async_remote_copy(
                src_ref=send.at[to],
                dst_ref=recv.at[g],
                send_sem=fwd_send.at[r],
                recv_sem=fwd_recv.at[r],
                device_id=(to, c),
                device_id_type=MESH,
            )
        )
    for copy in forward:
        copy.start()
    recv[g] = send[g]

    up = pltpu.make_async_remote_copy(
        src_ref=mag.at[:, pl.ds(0, rows), :],
        dst_ref=halo.at[0],
        send_sem=halo_sem.at[0],
        recv_sem=halo_sem.at[1],
        device_id=(lax.rem(g + 1, groups), c),
        device_id_type=MESH,
    )
    down = pltpu.make_async_remote_copy(
        src_ref=mag.at[:, pl.ds(0, rows), :],
        dst_ref=halo.at[1],
        send_sem=halo_sem.at[2],
        recv_sem=halo_sem.at[3],
        device_id=(lax.rem(g + groups - 1, groups), c),
        device_id_type=MESH,
    )

    @pl.when(g < groups - 1)
    def _():
        up.start()

    @pl.when(g > 0)
    def _():
        down.start()

    for copy in near:
        copy.wait()
    for copy in far:
        copy.wait_recv()
    loads[5].wait()
    table_rows = 6 * cells
    even_rows = 4 * cells
    lane0 = lax.broadcasted_iota(jnp.int32, (table_rows, half), 1) == 0
    even = lax.broadcasted_iota(jnp.int32, (table_rows, half), 0) < even_rows
    sign = jnp.where(even, 1.0, -1.0).astype(F32)
    for p in range(pairs):
        first = nwl[0, p].reshape(table_rows, 2 * half)
        mirror = nwl[1, p].reshape(table_rows, 2 * half)
        rev_first = jnp.dot(first, rv[...], preferred_element_type=F32)
        rev_mirror = jnp.dot(mirror, rv[...], preferred_element_type=F32)
        lo_first, hi_first = first[:, :half].astype(F32), first[:, half:].astype(F32)
        lo_mirror, hi_mirror = mirror[:, :half].astype(F32), mirror[:, half:].astype(F32)
        if p == 0:
            alone = ((2 * g + c) * pairs == 0).astype(F32)
            paired = 1.0 - alone
            of_first = alone * rev_first + paired * rev_mirror
            of_mirror = alone * rev_mirror + paired * rev_first
        else:
            of_first, of_mirror = rev_mirror, rev_first
        k_first = lo_first + sign * of_first
        k_mirror = lo_mirror + sign * of_mirror
        middle = hi_first + sign * hi_mirror
        if p == 0:
            i_first = jnp.where(lane0, alone * (2.0 * hi_first) + paired * k_first, k_first)
            i_mirror = jnp.where(lane0, alone * (2.0 * hi_mirror) + paired * middle, k_mirror)
            k_mirror = jnp.where(lane0, alone * k_mirror + paired * middle, k_mirror)
        else:
            k_mirror = jnp.where(lane0, middle, k_mirror)
            i_first, i_mirror = k_first, k_mirror
        kern[pl.ds(p, table_rows, stride=own), :] = k_first
        kern[pl.ds(pairs + p, table_rows, stride=own), :] = k_mirror
        base = table_rows * own
        kern[pl.ds(base + p, even_rows, stride=own), :] = i_first[:even_rows]
        kern[pl.ds(base + pairs + p, even_rows, stride=own), :] = i_mirror[:even_rows]

    for comp in range(3):
        full = mag[comp].astype(F32)
        centre = full[:rows]
        total = pltpu.roll(full, 1, 0)[:rows] + pltpu.roll(full, 2 * rows - 1, 0)[:rows]
        total = total + pltpu.roll(centre, 1, 1) + pltpu.roll(centre, 2 * half - 1, 1)
        lap[comp] = total - 4.0 * centre

    lane = lax.broadcasted_iota(jnp.int32, (own, half), 1)
    slot = lax.broadcasted_iota(jnp.int32, (own, half), 0)
    first_t = (2 * g + c) * pairs + lax.rem(slot, pairs)
    packed = jnp.logical_and(lane == 0, first_t > 0)
    at_first = jnp.logical_and(packed, slot < pairs)
    at_mirror = jnp.logical_and(packed, slot >= pairs)

    def flip(v):
        return jnp.concatenate([v[pairs:], v[:pairs]], axis=0)

    def unpack(j):
        block = recv[j].astype(F32)
        for comp in range(3):
            re = block[:, 2 * comp * half : (2 * comp + 1) * half]
            im = block[:, (2 * comp + 1) * half : (2 * comp + 2) * half]
            re_f, im_f = flip(re), flip(im)
            new_re = jnp.where(at_first, 0.5 * (re + re_f), jnp.where(at_mirror, 0.5 * (im + im_f), re))
            new_im = jnp.where(at_first, 0.5 * (im - im_f), jnp.where(at_mirror, 0.5 * (re - re_f), im))
            source[j, 2 * comp] = new_re
            source[j, 2 * comp + 1] = new_im

    unpack(g)
    for r in range(1, groups):
        forward[r - 1].wait_recv()
        unpack(lax.rem(g + groups - r, groups))

    def k_of(entry, d):
        start = pl.multiple_of((entry * cells + d) * own, own)
        return kern[pl.ds(start, own), :]

    def couple(i, carry):
        acc = [jnp.zeros((own, half), F32) for _ in range(6)]
        for j in range(cells):
            d = jnp.abs(i - j)
            s = jnp.where(i >= j, 1.0, -1.0).astype(F32)
            xx, yy, zz, yz = (k_of(e, d) for e in range(4))
            xy, xz = s * k_of(4, d), s * k_of(5, d)
            xxi, yyi, zzi, yzi = (k_of(6 + e, d) for e in range(4))
            xr, xi, yr, yim, zr, zim = (source[j, q] for q in range(6))
            acc[0] += xx * xr - xy * yim - xz * zim
            acc[1] += xxi * xi + xy * yr + xz * zr
            acc[2] += yy * yr + yz * zr - xy * xi
            acc[3] += yyi * yim + yzi * zim + xy * xr
            acc[4] += yz * yr + zz * zr - xz * xi
            acc[5] += yzi * yim + zzi * zim + xz * xr
        for comp in range(3):
            re, im = acc[2 * comp], acc[2 * comp + 1]
            re_f, im_f = flip(re), flip(im)
            new_re = jnp.where(at_first, re - im_f, jnp.where(at_mirror, re_f + im, re))
            new_im = jnp.where(at_first, im + re_f, jnp.where(at_mirror, re - im_f, im))
            back[i, :, pl.ds(2 * comp * half, half)] = new_re.astype(BF16)
            back[i, :, pl.ds((2 * comp + 1) * half, half)] = new_im.astype(BF16)
        return carry

    lax.fori_loop(0, cells, couple, 0)

    backward = []
    for r in range(1, groups):
        to = lax.rem(g + r, groups)
        backward.append(
            pltpu.make_async_remote_copy(
                src_ref=back.at[to],
                dst_ref=fields.at[c, g],
                send_sem=bwd_send.at[r],
                recv_sem=bwd_recv.at[r],
                device_id=(to, c),
                device_id_type=MESH,
            )
        )
    for copy in backward:
        copy.start()
    fields[c, g] = back[g]

    def relay(r):
        who = lax.rem(g + groups - r, groups)
        return pltpu.make_async_remote_copy(
            src_ref=fields.at[c, who],
            dst_ref=fields.at[c, who],
            send_sem=rel_send.at[r],
            recv_sem=rel_recv.at[r],
            device_id=(g, other),
            device_id_type=MESH,
        )

    relays = [relay(r) for r in range(groups)]
    relays[0].start()

    @pl.when(g == 0)
    def _():
        halo[0] = mag[:, pl.ds(0, rows), :]

    @pl.when(g > 0)
    def _():
        up.wait_recv()

    @pl.when(g == groups - 1)
    def _():
        halo[1] = mag[:, pl.ds(0, rows), :]

    @pl.when(g < groups - 1)
    def _():
        down.wait_recv()

    for comp in range(3):
        centre = mag[comp, pl.ds(0, rows), :].astype(F32)
        x_part = halo[0, comp].astype(F32) + halo[1, comp].astype(F32) - 2.0 * centre
        lap[comp] = EXCHANGE * (lap[comp] + x_part)

    for r in range(1, groups):
        backward[r - 1].wait_recv()
        relays[r].start()
    for r in range(groups):
        relays[r].wait_recv()
    for part in range(2):
        for i in range(groups):
            stack[pl.ds((part * groups + i) * own, own), :] = fields[part, i].astype(F32)

    loads[6].wait()
    loads[7].wait()
    scale = 1.0 / (2 * rows * 2 * half)
    writes = []
    for comp in range(3):
        modes = stack[:, pl.ds(2 * comp * half, 2 * half)].astype(BF16)
        cos_part = jnp.dot(yi[0], modes, preferred_element_type=F32)
        sin_part = jnp.dot(yi[1], modes, preferred_element_type=F32)
        g_rows = jnp.concatenate(
            [
                cos_part[:, :half] - sin_part[:, half:],
                cos_part[:, half:] + sin_part[:, :half],
            ],
            axis=1,
        ).astype(BF16)
        demag = jnp.dot(g_rows, zi[...], preferred_element_type=F32) * scale
        result[comp] = (demag + lap[comp]).astype(BF16)
        write = pltpu.make_async_copy(result.at[comp], out.at[comp], out_sem.at[comp])
        write.start()
        writes.append(write)

    for copy in swap + far + forward + backward + relays:
        copy.wait_send()

    @pl.when(g < groups - 1)
    def _():
        up.wait_send()

    @pl.when(g > 0)
    def _():
        down.wait_send()

    for write in writes:
        write.wait()


def on_device(magnet, newell, *consts):
    rows, _, x_cells, z_total = magnet.shape
    groups = lax.axis_size("gx")
    parts = lax.axis_size("yz")
    assert x_cells == 1 and parts == 2
    y_total = rows * parts
    pairs = y_total // (groups * parts * 2)
    own = 2 * pairs
    half = z_total // 2
    wide = 3 * z_total
    any_ref = pl.BlockSpec(memory_space=pl.ANY)
    dma = pltpu.SemaphoreType.DMA
    planes = jnp.transpose(magnet[:, :, 0, :], (1, 0, 2))
    field = pl.pallas_call(
        functools.partial(kernel, groups, pairs),
        out_shape=jax.ShapeDtypeStruct(planes.shape, BF16),
        in_specs=[any_ref] * 7,
        out_specs=any_ref,
        scratch_shapes=[
            pltpu.VMEM((3, y_total, z_total), BF16),
            pltpu.VMEM((2, pairs, 6, groups, z_total), BF16),
            pltpu.VMEM((2, rows, y_total), BF16),
            pltpu.VMEM((2, rows, y_total), BF16),
            pltpu.VMEM((z_total, z_total), BF16),
            pltpu.VMEM((z_total, z_total), BF16),
            pltpu.VMEM((z_total, half), BF16),
            pltpu.VMEM((2, 3, rows, z_total), BF16),
            pltpu.VMEM((rows, wide), F32),
            pltpu.VMEM((groups, own, wide), BF16),
            pltpu.VMEM((groups, own, wide), BF16),
            pltpu.VMEM((10 * groups * own, half), F32),
            pltpu.VMEM((groups, 6, own, half), F32),
            pltpu.VMEM((groups, own, wide), BF16),
            pltpu.VMEM((2, groups, own, wide), BF16),
            pltpu.VMEM((y_total, wide), F32),
            pltpu.VMEM((3, rows, z_total), F32),
            pltpu.VMEM((3, rows, z_total), BF16),
            dma((8,)),
            dma((pairs,)),
            dma((2, 3 + pairs)),
            dma((4,)),
            dma((groups,)),
            dma((groups,)),
            dma((groups,)),
            dma((groups,)),
            dma((groups,)),
            dma((groups,)),
            dma((3,)),
        ],
        compiler_params=pltpu.CompilerParams(collective_id=0, has_side_effects=True),
    )(planes, newell, *consts)
    return jnp.transpose(field, (1, 0, 2))[:, :, None, :]


def solution(mesh):
    groups, parts = mesh.shape["gx"], mesh.shape["yz"]

    def run(magnet, newell):
        consts = tables(groups, parts, magnet.shape[0], magnet.shape[3])
        body = lambda m, n: on_device(m, n, *[jnp.asarray(t) for t in consts])
        return jax.shard_map(
            body,
            mesh=mesh,
            in_specs=(P("yz", None, "gx", None), P("yz", None, None, None)),
            out_specs=P("yz", None, "gx", None),
            check_vma=False,
        )(magnet, newell)

    return run
```

```python
import functools
import math

import jax
import jax.numpy as jnp
import ml_dtypes
import numpy as np
from jax import lax
from jax.experimental import pallas as pl
from jax.experimental.pallas import tpu as pltpu
from jax.sharding import PartitionSpec as P

EXCHANGE = 0.2
F32 = jnp.float32
BF16 = jnp.bfloat16
MESH = pl.DeviceIdType.MESH


def ky_owned(groups, parts, pairs, length):
    order = []
    for part in range(parts):
        for g in range(groups):
            first = [(g * parts + part) * pairs + p for p in range(pairs)]
            mirror = [(length - t) if t else length // 2 for t in first]
            order.append(first + mirror)
    return np.array(order).reshape(parts, -1)


def tables(groups, parts, y_total, z_total):
    pairs = y_total // (groups * parts * 2)
    rows = y_total // parts
    order = ky_owned(groups, parts, pairs, y_total)

    def trig(k, n, length):
        angle = (k[:, None] * n[None, :] % length) * (2.0 * math.pi / length)
        return np.cos(angle), np.sin(angle)

    forward, inverse = [], []
    for part in range(parts):
        own_first = (np.arange(y_total) + part * rows) % y_total
        forward.append(np.stack(trig(order[part], own_first, y_total)))
        inverse.append(np.stack(trig(own_first[:rows], order.reshape(-1), y_total)))
    half = z_total // 2
    cos, sin = trig(np.arange(z_total), np.arange(half), z_total)
    alternate = np.cos(math.pi * np.arange(z_total))
    z_fwd = np.concatenate([cos, -sin], axis=1)
    z_fwd[:, half] = alternate
    z_inv = -np.concatenate([cos, -sin], axis=1).T
    z_inv[0] = -0.5
    z_inv[half] = -0.5 * alternate
    reverse = np.zeros((z_total, half))
    for k in range(half):
        reverse[-k % z_total, k] = 1.0
    cast = lambda a: np.asarray(a, np.float32).astype(ml_dtypes.bfloat16)
    return (
        cast(np.stack(forward)),
        cast(np.stack(inverse)),
        cast(z_fwd),
        cast(z_inv),
        cast(reverse),
    )


def kernel(
    groups, pairs, magnet, newell, y_fwd, y_inv, z_fwd, z_inv, rev, out,
    mag, nwl, yf, yi, zf, zi, rv, halo, spec, send, recv, kern, source, back, fields, stack,
    lap, result, load_sem, nwl_sem, pair_sem, halo_sem, fwd_send, fwd_recv, bwd_send, bwd_recv,
    rel_send, rel_recv, out_sem, hand,
):
    g = lax.axis_index("gx")
    c = lax.axis_index("yz")
    other = 1 - c
    own = 2 * pairs
    rows = magnet.shape[1]
    cells = groups
    half = magnet.shape[2] // 2

    plane = math.gcd(groups, 4)
    layers = groups // plane

    def target(k):
        layer, place = k // plane, lax.rem(k, plane)
        layer = jnp.where(2 * (g // plane) < layers, layers - 1 - layer, layer)
        return layer * plane + lax.rem(g + place, plane)

    barrier = pltpu.get_barrier_semaphore()

    @pl.when(c == 0)
    def _():
        pl.semaphore_signal(barrier, inc=1, device_id=(g, 1), device_id_type=MESH)

    loads = []
    for comp in range(3):
        loads.append(
            pltpu.make_async_copy(
                magnet.at[comp], mag.at[comp, pl.ds(0, rows), :], load_sem.at[comp]
            )
        )
    loads.append(pltpu.make_async_copy(z_fwd, zf, load_sem.at[3]))
    loads.append(pltpu.make_async_copy(y_fwd.at[c], yf, load_sem.at[4]))
    loads.append(pltpu.make_async_copy(rev, rv, load_sem.at[5]))
    loads.append(pltpu.make_async_copy(y_inv.at[c], yi, load_sem.at[6]))
    loads.append(pltpu.make_async_copy(z_inv, zi, load_sem.at[7]))
    for copy in loads:
        copy.start()

    def newell_row(part, p):
        t = (2 * g + part) * pairs + p
        return (1 - c) * t + c * lax.rem(rows - t, rows)

    near = [
        pltpu.make_async_copy(newell.at[newell_row(c, p)], nwl.at[c, p], nwl_sem.at[p])
        for p in range(pairs)
    ]
    for copy in near:
        copy.start()

    @pl.when(c == 1)
    def _():
        pl.semaphore_wait(barrier, 1)
        pl.semaphore_signal(hand.at[0], inc=1, device_id=(g, 0), device_id_type=MESH)

    @pl.when(c == 0)
    def _():
        pl.semaphore_wait(hand.at[0], 1)
        for r in range(1, groups):
            pl.semaphore_signal(
                barrier, inc=1, device_id=(lax.rem(g + r, groups), 0), device_id_type=MESH
            )

    for comp in range(3):
        loads[comp].wait()
    swap = []
    for comp in range(3):
        swap.append(
            pltpu.make_async_remote_copy(
                src_ref=mag.at[comp, pl.ds(0, rows), :],
                dst_ref=mag.at[comp, pl.ds(rows, rows), :],
                send_sem=pair_sem.at[0, comp],
                recv_sem=pair_sem.at[1, comp],
                device_id=(g, other),
                device_id_type=MESH,
            )
        )
    for copy in swap:
        copy.start()
    far = []
    for p in range(pairs):
        far.append(
            pltpu.make_async_remote_copy(
                src_ref=newell.at[newell_row(other, p)],
                dst_ref=nwl.at[c, p],
                send_sem=pair_sem.at[0, 3 + p],
                recv_sem=pair_sem.at[1, 3 + p],
                device_id=(g, other),
                device_id_type=MESH,
            )
        )
    for copy in far:
        copy.start()

    loads[3].wait()
    loads[4].wait()
    for comp in range(3):
        swap[comp].wait_recv()
        z_rows = jnp.dot(mag[comp], zf[...], preferred_element_type=F32).astype(BF16)
        cos_part = jnp.dot(yf[0], z_rows, preferred_element_type=F32)
        sin_part = jnp.dot(yf[1], z_rows, preferred_element_type=F32)
        low = 2 * comp * half
        spec[:, pl.ds(low, half)] = cos_part[:, :half] + sin_part[:, half:]
        spec[:, pl.ds(low + half, half)] = cos_part[:, half:] - sin_part[:, :half]
    for i in range(groups):
        send[i] = spec[pl.ds(i * own, own), :].astype(BF16)

    @pl.when(c == 0)
    def _():
        pl.semaphore_wait(barrier, groups - 1)
        pl.semaphore_signal(hand.at[1], inc=1, device_id=(g, 1), device_id_type=MESH)

    @pl.when(c == 1)
    def _():
        pl.semaphore_wait(hand.at[1], 1)

    def forward(i):
        r = lax.rem(i - g + groups, groups)
        return pltpu.make_async_remote_copy(
            src_ref=send.at[i],
            dst_ref=recv.at[g],
            send_sem=fwd_send.at[r],
            recv_sem=fwd_recv.at[r],
            device_id=(i, c),
            device_id_type=MESH,
        )

    def arrival(buffer, sems, who):
        r = lax.rem(g - who + groups, groups)
        return pltpu.make_async_remote_copy(
            src_ref=buffer.at[who],
            dst_ref=buffer.at[who],
            send_sem=fwd_send.at[r],
            recv_sem=sems.at[r],
            device_id=(who, c),
            device_id_type=MESH,
        )

    for k in range(groups):
        @pl.when(target(k) != g)
        def _():
            forward(target(k)).start()

    recv[g] = send[g]

    up = pltpu.make_async_remote_copy(
        src_ref=mag.at[:, pl.ds(0, rows), :],
        dst_ref=halo.at[0],
        send_sem=halo_sem.at[0],
        recv_sem=halo_sem.at[1],
        device_id=(lax.rem(g + 1, groups), c),
        device_id_type=MESH,
    )
    down = pltpu.make_async_remote_copy(
        src_ref=mag.at[:, pl.ds(0, rows), :],
        dst_ref=halo.at[1],
        send_sem=halo_sem.at[2],
        recv_sem=halo_sem.at[3],
        device_id=(lax.rem(g + groups - 1, groups), c),
        device_id_type=MESH,
    )

    @pl.when(g < groups - 1)
    def _():
        up.start()

    @pl.when(g > 0)
    def _():
        down.start()

    for copy in near:
        copy.wait()
    for copy in far:
        copy.wait_recv()
    loads[5].wait()
    table_rows = 6 * cells
    even_rows = 4 * cells
    lane0 = lax.broadcasted_iota(jnp.int32, (table_rows, half), 1) == 0
    even = lax.broadcasted_iota(jnp.int32, (table_rows, half), 0) < even_rows
    sign = jnp.where(even, 1.0, -1.0).astype(F32)
    for p in range(pairs):
        first = nwl[0, p].reshape(table_rows, 2 * half)
        mirror = nwl[1, p].reshape(table_rows, 2 * half)
        rev_first = jnp.dot(first, rv[...], preferred_element_type=F32)
        rev_mirror = jnp.dot(mirror, rv[...], preferred_element_type=F32)
        lo_first, hi_first = first[:, :half].astype(F32), first[:, half:].astype(F32)
        lo_mirror, hi_mirror = mirror[:, :half].astype(F32), mirror[:, half:].astype(F32)
        if p == 0:
            alone = ((2 * g + c) * pairs == 0).astype(F32)
            paired = 1.0 - alone
            of_first = alone * rev_first + paired * rev_mirror
            of_mirror = alone * rev_mirror + paired * rev_first
        else:
            of_first, of_mirror = rev_mirror, rev_first
        k_first = lo_first + sign * of_first
        k_mirror = lo_mirror + sign * of_mirror
        middle = hi_first + sign * hi_mirror
        if p == 0:
            i_first = jnp.where(lane0, alone * (2.0 * hi_first) + paired * k_first, k_first)
            i_mirror = jnp.where(lane0, alone * (2.0 * hi_mirror) + paired * middle, k_mirror)
            k_mirror = jnp.where(lane0, alone * k_mirror + paired * middle, k_mirror)
        else:
            k_mirror = jnp.where(lane0, middle, k_mirror)
            i_first, i_mirror = k_first, k_mirror
        kern[pl.ds(p, table_rows, stride=own), :] = k_first
        kern[pl.ds(pairs + p, table_rows, stride=own), :] = k_mirror
        base = table_rows * own
        kern[pl.ds(base + p, even_rows, stride=own), :] = i_first[:even_rows]
        kern[pl.ds(base + pairs + p, even_rows, stride=own), :] = i_mirror[:even_rows]

    for comp in range(3):
        full = mag[comp].astype(F32)
        centre = full[:rows]
        total = pltpu.roll(full, 1, 0)[:rows] + pltpu.roll(full, 2 * rows - 1, 0)[:rows]
        total = total + pltpu.roll(centre, 1, 1) + pltpu.roll(centre, 2 * half - 1, 1)
        lap[comp] = total - 4.0 * centre

    lane = lax.broadcasted_iota(jnp.int32, (own, half), 1)
    slot = lax.broadcasted_iota(jnp.int32, (own, half), 0)
    first_t = (2 * g + c) * pairs + lax.rem(slot, pairs)
    packed = jnp.logical_and(lane == 0, first_t > 0)
    at_first = jnp.logical_and(packed, slot < pairs)
    at_mirror = jnp.logical_and(packed, slot >= pairs)

    def flip(v):
        return jnp.concatenate([v[pairs:], v[:pairs]], axis=0)

    def unpack(j):
        block = recv[j].astype(F32)
        for comp in range(3):
            re = block[:, 2 * comp * half : (2 * comp + 1) * half]
            im = block[:, (2 * comp + 1) * half : (2 * comp + 2) * half]
            re_f, im_f = flip(re), flip(im)
            new_re = jnp.where(at_first, 0.5 * (re + re_f), jnp.where(at_mirror, 0.5 * (im + im_f), re))
            new_im = jnp.where(at_first, 0.5 * (im - im_f), jnp.where(at_mirror, 0.5 * (re - re_f), im))
            source[j, 2 * comp] = new_re
            source[j, 2 * comp + 1] = new_im

    for k in range(groups - 1, -1, -1):
        who = target(k)

        @pl.when(who != g)
        def _():
            arrival(recv, fwd_recv, who).wait_recv()

        unpack(who)

    def k_of(entry, d):
        start = pl.multiple_of((entry * cells + d) * own, own)
        return kern[pl.ds(start, own), :]

    def backward(i):
        r = lax.rem(i - g + groups, groups)
        return pltpu.make_async_remote_copy(
            src_ref=back.at[i],
            dst_ref=fields.at[c, g],
            send_sem=bwd_send.at[r],
            recv_sem=bwd_recv.at[r],
            device_id=(i, c),
            device_id_type=MESH,
        )

    def couple(k, carry):
        i = target(k)
        acc = [jnp.zeros((own, half), F32) for _ in range(6)]
        for j in range(cells):
            d = jnp.abs(i - j)
            s = jnp.where(i >= j, 1.0, -1.0).astype(F32)
            xx, yy, zz, yz = (k_of(e, d) for e in range(4))
            xy, xz = s * k_of(4, d), s * k_of(5, d)
            xxi, yyi, zzi, yzi = (k_of(6 + e, d) for e in range(4))
            xr, xi, yr, yim, zr, zim = (source[j, q] for q in range(6))
            acc[0] += xx * xr - xy * yim - xz * zim
            acc[1] += xxi * xi + xy * yr + xz * zr
            acc[2] += yy * yr + yz * zr - xy * xi
            acc[3] += yyi * yim + yzi * zim + xy * xr
            acc[4] += yz * yr + zz * zr - xz * xi
            acc[5] += yzi * yim + zzi * zim + xz * xr
        for comp in range(3):
            re, im = acc[2 * comp], acc[2 * comp + 1]
            re_f, im_f = flip(re), flip(im)
            new_re = jnp.where(at_first, re - im_f, jnp.where(at_mirror, re_f + im, re))
            new_im = jnp.where(at_first, im + re_f, jnp.where(at_mirror, re - im_f, im))
            back[i, :, pl.ds(2 * comp * half, half)] = new_re.astype(BF16)
            back[i, :, pl.ds((2 * comp + 1) * half, half)] = new_im.astype(BF16)
        before = target(jnp.maximum(k - 1, 0))

        @pl.when(jnp.logical_and(k > 0, before != g))
        def _():
            backward(before).start()

        return carry

    lax.fori_loop(0, cells, couple, 0)

    @pl.when(target(groups - 1) != g)
    def _():
        backward(target(groups - 1)).start()

    fields[c, g] = back[g]

    def relay(who):
        return pltpu.make_async_remote_copy(
            src_ref=fields.at[c, who],
            dst_ref=fields.at[c, who],
            send_sem=rel_send.at[who],
            recv_sem=rel_recv.at[who],
            device_id=(g, other),
            device_id_type=MESH,
        )

    @pl.when(g == 0)
    def _():
        halo[0] = mag[:, pl.ds(0, rows), :]

    @pl.when(g > 0)
    def _():
        up.wait_recv()

    @pl.when(g == groups - 1)
    def _():
        halo[1] = mag[:, pl.ds(0, rows), :]

    @pl.when(g < groups - 1)
    def _():
        down.wait_recv()

    for comp in range(3):
        centre = mag[comp, pl.ds(0, rows), :].astype(F32)
        x_part = halo[0, comp].astype(F32) + halo[1, comp].astype(F32) - 2.0 * centre
        lap[comp] = EXCHANGE * (lap[comp] + x_part)

    for k in range(groups - 1, -1, -1):
        who = target(k)

        @pl.when(who != g)
        def _():
            arrival(fields.at[c], bwd_recv, who).wait_recv()

        relay(who).start()
    for i in range(groups):
        relay(i).wait_recv()
    for part in range(2):
        for i in range(groups):
            stack[pl.ds((part * groups + i) * own, own), :] = fields[part, i].astype(F32)

    loads[6].wait()
    loads[7].wait()
    scale = 1.0 / (2 * rows * 2 * half)
    writes = []
    for comp in range(3):
        modes = stack[:, pl.ds(2 * comp * half, 2 * half)].astype(BF16)
        cos_part = jnp.dot(yi[0], modes, preferred_element_type=F32)
        sin_part = jnp.dot(yi[1], modes, preferred_element_type=F32)
        g_rows = jnp.concatenate(
            [
                cos_part[:, :half] - sin_part[:, half:],
                cos_part[:, half:] + sin_part[:, :half],
            ],
            axis=1,
        ).astype(BF16)
        demag = jnp.dot(g_rows, zi[...], preferred_element_type=F32) * scale
        result[comp] = (demag + lap[comp]).astype(BF16)
        write = pltpu.make_async_copy(result.at[comp], out.at[comp], out_sem.at[comp])
        write.start()
        writes.append(write)

    for copy in swap + far:
        copy.wait_send()
    for i in range(groups):
        relay(i).wait_send()

        @pl.when(i != g)
        def _():
            forward(i).wait_send()
            backward(i).wait_send()

    @pl.when(g < groups - 1)
    def _():
        up.wait_send()

    @pl.when(g > 0)
    def _():
        down.wait_send()

    for write in writes:
        write.wait()


def on_device(magnet, newell, *consts):
    rows, _, x_cells, z_total = magnet.shape
    groups = lax.axis_size("gx")
    parts = lax.axis_size("yz")
    assert x_cells == 1 and parts == 2
    y_total = rows * parts
    pairs = y_total // (groups * parts * 2)
    own = 2 * pairs
    half = z_total // 2
    wide = 3 * z_total
    any_ref = pl.BlockSpec(memory_space=pl.ANY)
    dma = pltpu.SemaphoreType.DMA
    planes = jnp.transpose(magnet[:, :, 0, :], (1, 0, 2))
    field = pl.pallas_call(
        functools.partial(kernel, groups, pairs),
        out_shape=jax.ShapeDtypeStruct(planes.shape, BF16),
        in_specs=[any_ref] * 7,
        out_specs=any_ref,
        scratch_shapes=[
            pltpu.VMEM((3, y_total, z_total), BF16),
            pltpu.VMEM((2, pairs, 6, groups, z_total), BF16),
            pltpu.VMEM((2, rows, y_total), BF16),
            pltpu.VMEM((2, rows, y_total), BF16),
            pltpu.VMEM((z_total, z_total), BF16),
            pltpu.VMEM((z_total, z_total), BF16),
            pltpu.VMEM((z_total, half), BF16),
            pltpu.VMEM((2, 3, rows, z_total), BF16),
            pltpu.VMEM((rows, wide), F32),
            pltpu.VMEM((groups, own, wide), BF16),
            pltpu.VMEM((groups, own, wide), BF16),
            pltpu.VMEM((10 * groups * own, half), F32),
            pltpu.VMEM((groups, 6, own, half), F32),
            pltpu.VMEM((groups, own, wide), BF16),
            pltpu.VMEM((2, groups, own, wide), BF16),
            pltpu.VMEM((y_total, wide), F32),
            pltpu.VMEM((3, rows, z_total), F32),
            pltpu.VMEM((3, rows, z_total), BF16),
            dma((8,)),
            dma((pairs,)),
            dma((2, 3 + pairs)),
            dma((4,)),
            dma((groups,)),
            dma((groups,)),
            dma((groups,)),
            dma((groups,)),
            dma((groups,)),
            dma((groups,)),
            dma((3,)),
            pltpu.SemaphoreType.REGULAR((2,)),
        ],
        compiler_params=pltpu.CompilerParams(collective_id=0, has_side_effects=True),
    )(planes, newell, *consts)
    return jnp.transpose(field, (1, 0, 2))[:, :, None, :]


def solution(mesh):
    groups, parts = mesh.shape["gx"], mesh.shape["yz"]

    def run(magnet, newell):
        consts = tables(groups, parts, magnet.shape[0], magnet.shape[3])
        body = lambda m, n: on_device(m, n, *[jnp.asarray(t) for t in consts])
        return jax.shard_map(
            body,
            mesh=mesh,
            in_specs=(P("yz", None, "gx", None), P("yz", None, None, None)),
            out_specs=P("yz", None, "gx", None),
            check_vma=False,
        )(magnet, newell)

    return run
```

```python
import functools
import math

import jax
import jax.numpy as jnp
import ml_dtypes
import numpy as np
from jax import lax
from jax.experimental import pallas as pl
from jax.experimental.pallas import tpu as pltpu
from jax.sharding import PartitionSpec as P

EXCHANGE = 0.2
F32 = jnp.float32
BF16 = jnp.bfloat16
MESH = pl.DeviceIdType.MESH


def ky_owned(groups, parts, pairs, length):
    order = []
    for part in range(parts):
        for g in range(groups):
            first = [(g * parts + part) * pairs + p for p in range(pairs)]
            mirror = [(length - t) if t else length // 2 for t in first]
            order.append(first + mirror)
    return np.array(order).reshape(parts, -1)


def tables(groups, parts, y_total, z_total):
    pairs = y_total // (groups * parts * 2)
    rows = y_total // parts
    order = ky_owned(groups, parts, pairs, y_total)

    def trig(k, n, length):
        angle = (k[:, None] * n[None, :] % length) * (2.0 * math.pi / length)
        return np.cos(angle), np.sin(angle)

    forward, inverse = [], []
    for part in range(parts):
        own_first = (np.arange(y_total) + part * rows) % y_total
        forward.append(np.stack(trig(order[part], own_first, y_total)))
        inverse.append(np.stack(trig(own_first[:rows], order.reshape(-1), y_total)))
    half = z_total // 2
    cos, sin = trig(np.arange(z_total), np.arange(half), z_total)
    alternate = np.cos(math.pi * np.arange(z_total))
    z_fwd = np.concatenate([cos, -sin], axis=1)
    z_fwd[:, half] = alternate
    z_inv = -np.concatenate([cos, -sin], axis=1).T
    z_inv[0] = -0.5
    z_inv[half] = -0.5 * alternate
    reverse = np.zeros((z_total, half))
    for k in range(half):
        reverse[-k % z_total, k] = 1.0
    cast = lambda a: np.asarray(a, np.float32).astype(ml_dtypes.bfloat16)
    return (
        cast(np.stack(forward)),
        cast(np.stack(inverse)),
        cast(z_fwd),
        cast(z_inv),
        cast(reverse),
    )


def kernel(
    groups, pairs, magnet, newell, y_fwd, y_inv, z_fwd, z_inv, rev, out,
    mag, nwl, yf, yi, zf, zi, rv, halo, spec, send, recv, kern, source, back, fields, stack,
    lap, load_sem, nwl_sem, pair_sem, halo_sem, fwd_send, fwd_recv, bwd_send, bwd_recv,
    rel_send, rel_recv, hand,
):
    g = lax.axis_index("gx")
    c = lax.axis_index("yz")
    other = 1 - c
    own = 2 * pairs
    rows = magnet.shape[1]
    cells = groups
    half = magnet.shape[2] // 2

    plane = math.gcd(groups, 4)
    layers = groups // plane

    def target(k):
        layer, place = k // plane, lax.rem(k, plane)
        layer = jnp.where(2 * (g // plane) < layers, layers - 1 - layer, layer)
        return layer * plane + lax.rem(g + place, plane)

    barrier = pltpu.get_barrier_semaphore()

    @pl.when(c == 0)
    def _():
        pl.semaphore_signal(barrier, inc=1, device_id=(g, 1), device_id_type=MESH)

    loads = []
    for comp in range(3):
        loads.append(
            pltpu.make_async_copy(
                magnet.at[comp], mag.at[comp, pl.ds(0, rows), :], load_sem.at[comp]
            )
        )
    loads.append(pltpu.make_async_copy(z_fwd, zf, load_sem.at[3]))
    loads.append(pltpu.make_async_copy(y_fwd.at[c], yf, load_sem.at[4]))
    loads.append(pltpu.make_async_copy(rev, rv, load_sem.at[5]))
    loads.append(pltpu.make_async_copy(y_inv.at[c], yi, load_sem.at[6]))
    loads.append(pltpu.make_async_copy(z_inv, zi, load_sem.at[7]))
    for copy in loads:
        copy.start()

    def newell_row(part, p):
        t = (2 * g + part) * pairs + p
        return (1 - c) * t + c * lax.rem(rows - t, rows)

    near = [
        pltpu.make_async_copy(newell.at[newell_row(c, p)], nwl.at[c, p], nwl_sem.at[p])
        for p in range(pairs)
    ]
    for copy in near:
        copy.start()

    @pl.when(c == 1)
    def _():
        pl.semaphore_wait(barrier, 1)
        pl.semaphore_signal(hand.at[0], inc=1, device_id=(g, 0), device_id_type=MESH)

    @pl.when(c == 0)
    def _():
        pl.semaphore_wait(hand.at[0], 1)
        for r in range(1, groups):
            pl.semaphore_signal(
                barrier, inc=1, device_id=(lax.rem(g + r, groups), 0), device_id_type=MESH
            )

    for comp in range(3):
        loads[comp].wait()
    swap = []
    for comp in range(3):
        swap.append(
            pltpu.make_async_remote_copy(
                src_ref=mag.at[comp, pl.ds(0, rows), :],
                dst_ref=mag.at[comp, pl.ds(rows, rows), :],
                send_sem=pair_sem.at[0, comp],
                recv_sem=pair_sem.at[1, comp],
                device_id=(g, other),
                device_id_type=MESH,
            )
        )
    for copy in swap:
        copy.start()
    far = []
    for p in range(pairs):
        far.append(
            pltpu.make_async_remote_copy(
                src_ref=newell.at[newell_row(other, p)],
                dst_ref=nwl.at[c, p],
                send_sem=pair_sem.at[0, 3 + p],
                recv_sem=pair_sem.at[1, 3 + p],
                device_id=(g, other),
                device_id_type=MESH,
            )
        )
    for copy in far:
        copy.start()

    loads[3].wait()
    loads[4].wait()
    for comp in range(3):
        swap[comp].wait_recv()
        z_rows = jnp.dot(mag[comp], zf[...], preferred_element_type=F32).astype(BF16)
        cos_part = jnp.dot(yf[0], z_rows, preferred_element_type=F32)
        sin_part = jnp.dot(yf[1], z_rows, preferred_element_type=F32)
        low = 2 * comp * half
        spec[:, pl.ds(low, half)] = cos_part[:, :half] + sin_part[:, half:]
        spec[:, pl.ds(low + half, half)] = cos_part[:, half:] - sin_part[:, :half]
    for i in range(groups):
        send[i] = spec[pl.ds(i * own, own), :].astype(BF16)

    @pl.when(c == 0)
    def _():
        pl.semaphore_wait(barrier, groups - 1)
        pl.semaphore_signal(hand.at[1], inc=1, device_id=(g, 1), device_id_type=MESH)

    @pl.when(c == 1)
    def _():
        pl.semaphore_wait(hand.at[1], 1)

    def forward(i):
        r = lax.rem(i - g + groups, groups)
        return pltpu.make_async_remote_copy(
            src_ref=send.at[i],
            dst_ref=recv.at[g],
            send_sem=fwd_send.at[r],
            recv_sem=fwd_recv.at[r],
            device_id=(i, c),
            device_id_type=MESH,
        )

    def arrival(buffer, sems, who):
        r = lax.rem(g - who + groups, groups)
        return pltpu.make_async_remote_copy(
            src_ref=buffer.at[who],
            dst_ref=buffer.at[who],
            send_sem=fwd_send.at[r],
            recv_sem=sems.at[r],
            device_id=(who, c),
            device_id_type=MESH,
        )

    for k in range(groups):
        @pl.when(target(k) != g)
        def _():
            forward(target(k)).start()

    recv[g] = send[g]

    def halo_copy(side, comp):
        to = lax.rem(g + (1, groups - 1)[side], groups)
        return pltpu.make_async_remote_copy(
            src_ref=mag.at[comp, pl.ds(0, rows), :],
            dst_ref=halo.at[side, comp],
            send_sem=halo_sem.at[0, side, comp],
            recv_sem=halo_sem.at[1, side, comp],
            device_id=(to, c),
            device_id_type=MESH,
        )

    has_next, has_last = g < groups - 1, g > 0

    def halo_start(comps):
        @pl.when(has_next)
        def _():
            for comp in comps:
                halo_copy(0, comp).start()

        @pl.when(has_last)
        def _():
            for comp in comps:
                halo_copy(1, comp).start()

    halo_start((0, 1))

    for copy in near:
        copy.wait()
    for copy in far:
        copy.wait_recv()
    loads[5].wait()
    table_rows = 6 * cells
    even_rows = 4 * cells
    lane0 = lax.broadcasted_iota(jnp.int32, (table_rows, half), 1) == 0
    even = lax.broadcasted_iota(jnp.int32, (table_rows, half), 0) < even_rows
    sign = jnp.where(even, 1.0, -1.0).astype(F32)
    for p in range(pairs):
        first = nwl[0, p].reshape(table_rows, 2 * half)
        mirror = nwl[1, p].reshape(table_rows, 2 * half)
        rev_first = jnp.dot(first, rv[...], preferred_element_type=F32)
        rev_mirror = jnp.dot(mirror, rv[...], preferred_element_type=F32)
        lo_first, hi_first = first[:, :half].astype(F32), first[:, half:].astype(F32)
        lo_mirror, hi_mirror = mirror[:, :half].astype(F32), mirror[:, half:].astype(F32)
        if p == 0:
            alone = ((2 * g + c) * pairs == 0).astype(F32)
            paired = 1.0 - alone
            of_first = alone * rev_first + paired * rev_mirror
            of_mirror = alone * rev_mirror + paired * rev_first
        else:
            of_first, of_mirror = rev_mirror, rev_first
        k_first = lo_first + sign * of_first
        k_mirror = lo_mirror + sign * of_mirror
        middle = hi_first + sign * hi_mirror
        if p == 0:
            i_first = jnp.where(lane0, alone * (2.0 * hi_first) + paired * k_first, k_first)
            i_mirror = jnp.where(lane0, alone * (2.0 * hi_mirror) + paired * middle, k_mirror)
            k_mirror = jnp.where(lane0, alone * k_mirror + paired * middle, k_mirror)
        else:
            k_mirror = jnp.where(lane0, middle, k_mirror)
            i_first, i_mirror = k_first, k_mirror
        kern[pl.ds(p, table_rows, stride=own), :] = k_first
        kern[pl.ds(pairs + p, table_rows, stride=own), :] = k_mirror
        base = table_rows * own
        kern[pl.ds(base + p, even_rows, stride=own), :] = i_first[:even_rows]
        kern[pl.ds(base + pairs + p, even_rows, stride=own), :] = i_mirror[:even_rows]

    for comp in range(3):
        full = mag[comp].astype(F32)
        centre = full[:rows]
        total = pltpu.roll(full, 1, 0)[:rows] + pltpu.roll(full, 2 * rows - 1, 0)[:rows]
        total = total + pltpu.roll(centre, 1, 1) + pltpu.roll(centre, 2 * half - 1, 1)
        lap[comp] = total - 4.0 * centre

    lane = lax.broadcasted_iota(jnp.int32, (own, half), 1)
    slot = lax.broadcasted_iota(jnp.int32, (own, half), 0)
    first_t = (2 * g + c) * pairs + lax.rem(slot, pairs)
    packed = jnp.logical_and(lane == 0, first_t > 0)
    at_first = jnp.logical_and(packed, slot < pairs)
    at_mirror = jnp.logical_and(packed, slot >= pairs)

    def flip(v):
        return jnp.concatenate([v[pairs:], v[:pairs]], axis=0)

    def unpack(j):
        block = recv[j].astype(F32)
        for comp in range(3):
            re = block[:, 2 * comp * half : (2 * comp + 1) * half]
            im = block[:, (2 * comp + 1) * half : (2 * comp + 2) * half]
            re_f, im_f = flip(re), flip(im)
            new_re = jnp.where(at_first, 0.5 * (re + re_f), jnp.where(at_mirror, 0.5 * (im + im_f), re))
            new_im = jnp.where(at_first, 0.5 * (im - im_f), jnp.where(at_mirror, 0.5 * (re - re_f), im))
            source[j, 2 * comp] = new_re
            source[j, 2 * comp + 1] = new_im

    for k in range(groups - 1, -1, -1):
        who = target(k)

        @pl.when(who != g)
        def _():
            arrival(recv, fwd_recv, who).wait_recv()

        unpack(who)

    def k_of(entry, d):
        start = pl.multiple_of((entry * cells + d) * own, own)
        return kern[pl.ds(start, own), :]

    def backward(i):
        r = lax.rem(i - g + groups, groups)
        return pltpu.make_async_remote_copy(
            src_ref=back.at[i],
            dst_ref=fields.at[c, g],
            send_sem=bwd_send.at[r],
            recv_sem=bwd_recv.at[r],
            device_id=(i, c),
            device_id_type=MESH,
        )

    def couple(k, carry):
        i = target(k)
        acc = [jnp.zeros((own, half), F32) for _ in range(6)]
        for j in range(cells):
            d = jnp.abs(i - j)
            s = jnp.where(i >= j, 1.0, -1.0).astype(F32)
            xx, yy, zz, yz = (k_of(e, d) for e in range(4))
            xy, xz = s * k_of(4, d), s * k_of(5, d)
            xxi, yyi, zzi, yzi = (k_of(6 + e, d) for e in range(4))
            xr, xi, yr, yim, zr, zim = (source[j, q] for q in range(6))
            acc[0] += xx * xr - xy * yim - xz * zim
            acc[1] += xxi * xi + xy * yr + xz * zr
            acc[2] += yy * yr + yz * zr - xy * xi
            acc[3] += yyi * yim + yzi * zim + xy * xr
            acc[4] += yz * yr + zz * zr - xz * xi
            acc[5] += yzi * yim + zzi * zim + xz * xr
        for comp in range(3):
            re, im = acc[2 * comp], acc[2 * comp + 1]
            re_f, im_f = flip(re), flip(im)
            new_re = jnp.where(at_first, re - im_f, jnp.where(at_mirror, re_f + im, re))
            new_im = jnp.where(at_first, im + re_f, jnp.where(at_mirror, re - im_f, im))
            back[i, :, pl.ds(2 * comp * half, half)] = new_re.astype(BF16)
            back[i, :, pl.ds((2 * comp + 1) * half, half)] = new_im.astype(BF16)
        before = target(jnp.maximum(k - 1, 0))

        @pl.when(jnp.logical_and(k > 0, before != g))
        def _():
            backward(before).start()

        return carry

    lax.fori_loop(0, cells, couple, 0)

    @pl.when(target(groups - 1) != g)
    def _():
        backward(target(groups - 1)).start()

    halo_start((2,))
    fields[c, g] = back[g]

    def relay(who):
        return pltpu.make_async_remote_copy(
            src_ref=fields.at[c, who],
            dst_ref=fields.at[c, who],
            send_sem=rel_send.at[who],
            recv_sem=rel_recv.at[who],
            device_id=(g, other),
            device_id_type=MESH,
        )

    for k in range(groups - 1, -1, -1):
        who = target(k)

        @pl.when(who != g)
        def _():
            arrival(fields.at[c], bwd_recv, who).wait_recv()

        relay(who).start()
    for side, inside in enumerate((has_last, has_next)):
        @pl.when(inside)
        def _():
            for comp in range(3):
                halo_copy(side, comp).wait_recv()

        @pl.when(jnp.logical_not(inside))
        def _():
            halo[side] = mag[:, pl.ds(0, rows), :]

    for comp in range(3):
        centre = mag[comp, pl.ds(0, rows), :].astype(F32)
        x_part = halo[0, comp].astype(F32) + halo[1, comp].astype(F32) - 2.0 * centre
        lap[comp] = EXCHANGE * (lap[comp] + x_part)

    for i in range(groups):
        relay(i).wait_recv()
    for part in range(2):
        for i in range(groups):
            stack[pl.ds((part * groups + i) * own, own), :] = fields[part, i].astype(F32)

    loads[6].wait()
    loads[7].wait()
    scale = 1.0 / (2 * rows * 2 * half)
    for comp in range(3):
        modes = stack[:, pl.ds(2 * comp * half, 2 * half)].astype(BF16)
        cos_part = jnp.dot(yi[0], modes, preferred_element_type=F32)
        sin_part = jnp.dot(yi[1], modes, preferred_element_type=F32)
        g_rows = jnp.concatenate(
            [
                cos_part[:, :half] - sin_part[:, half:],
                cos_part[:, half:] + sin_part[:, :half],
            ],
            axis=1,
        ).astype(BF16)
        demag = jnp.dot(g_rows, zi[...], preferred_element_type=F32) * scale
        out[comp] = (demag + lap[comp]).astype(BF16)

    for copy in swap + far:
        copy.wait_send()
    for i in range(groups):
        relay(i).wait_send()

        @pl.when(i != g)
        def _():
            forward(i).wait_send()
            backward(i).wait_send()

    for side, inside in enumerate((has_next, has_last)):
        @pl.when(inside)
        def _():
            for comp in range(3):
                halo_copy(side, comp).wait_send()


def on_device(magnet, newell, *consts):
    rows, _, x_cells, z_total = magnet.shape
    groups = lax.axis_size("gx")
    parts = lax.axis_size("yz")
    assert x_cells == 1 and parts == 2
    y_total = rows * parts
    pairs = y_total // (groups * parts * 2)
    own = 2 * pairs
    half = z_total // 2
    wide = 3 * z_total
    any_ref = pl.BlockSpec(memory_space=pl.ANY)
    dma = pltpu.SemaphoreType.DMA
    planes = jnp.transpose(magnet[:, :, 0, :], (1, 0, 2))
    field = pl.pallas_call(
        functools.partial(kernel, groups, pairs),
        out_shape=pltpu.VMEM(planes.shape, BF16),
        in_specs=[any_ref] * 7,
        out_specs=pl.BlockSpec(memory_space=pltpu.VMEM),
        scratch_shapes=[
            pltpu.VMEM((3, y_total, z_total), BF16),
            pltpu.VMEM((2, pairs, 6, groups, z_total), BF16),
            pltpu.VMEM((2, rows, y_total), BF16),
            pltpu.VMEM((2, rows, y_total), BF16),
            pltpu.VMEM((z_total, z_total), BF16),
            pltpu.VMEM((z_total, z_total), BF16),
            pltpu.VMEM((z_total, half), BF16),
            pltpu.VMEM((2, 3, rows, z_total), BF16),
            pltpu.VMEM((rows, wide), F32),
            pltpu.VMEM((groups, own, wide), BF16),
            pltpu.VMEM((groups, own, wide), BF16),
            pltpu.VMEM((10 * groups * own, half), F32),
            pltpu.VMEM((groups, 6, own, half), F32),
            pltpu.VMEM((groups, own, wide), BF16),
            pltpu.VMEM((2, groups, own, wide), BF16),
            pltpu.VMEM((y_total, wide), F32),
            pltpu.VMEM((3, rows, z_total), F32),
            dma((8,)),
            dma((pairs,)),
            dma((2, 3 + pairs)),
            dma((2, 2, 3)),
            dma((groups,)),
            dma((groups,)),
            dma((groups,)),
            dma((groups,)),
            dma((groups,)),
            dma((groups,)),
            pltpu.SemaphoreType.REGULAR((2,)),
        ],
        compiler_params=pltpu.CompilerParams(collective_id=0, has_side_effects=True),
    )(planes, newell, *consts)
    return jnp.transpose(field, (1, 0, 2))[:, :, None, :]


def solution(mesh):
    groups, parts = mesh.shape["gx"], mesh.shape["yz"]

    def run(magnet, newell):
        consts = tables(groups, parts, magnet.shape[0], magnet.shape[3])
        body = lambda m, n: on_device(m, n, *[jnp.asarray(t) for t in consts])
        return jax.shard_map(
            body,
            mesh=mesh,
            in_specs=(P("yz", None, "gx", None), P("yz", None, None, None)),
            out_specs=P("yz", None, "gx", None),
            check_vma=False,
        )(magnet, newell)

    return run
```
